8 devices in a mesh: dy: 4 (over z, y, x), dx: 2 (over core).
Axes of the slice: x: 2, y: 2, z: 1, core: 2. Of those that a mesh axis runs over, the one named last changes fastest.
Arguments:
- tokens: bfloat16 [16384, 1024], P(('dy', 'dx'))
- targets: bfloat16 [16384, 1024], P(('dy', 'dx'))
- w_in: bfloat16 [4, 1024, 4096], replicated
- w_out: bfloat16 [4, 4096, 1024], replicated
Outputs:
- output 1: float32 [4, 1024, 4096], replicated
- output 2: float32 [4, 4096, 1024], replicated
All inputs are finite; a program needn't handle non-finite values.
Results may differ from the reference program's by a relative error of at most 0.00929466.
Values are sent between devices in bfloat16 or wider.
A program may use at most 1 GiB of HBM per device.

```python
import jax
import jax.numpy as jnp
from jax import lax

D = 1024
FF = 4096
TOK = 2048
LAYERS = 4
SHARDS = 8


def setup_inputs(seed: int = 0) -> dict:
    total_tok = SHARDS * TOK
    rng_keys = jax.random.split(jax.random.key(seed), 4)
    targ_scale = 0.5 * total_tok ** 0.5
    tokens = jax.random.normal(rng_keys[0], (total_tok, D), jnp.float32)
    targets = jax.random.normal(rng_keys[1], (total_tok, D), jnp.float32) * targ_scale
    w_in = jax.random.normal(rng_keys[2], (LAYERS, D, FF), jnp.float32) * D ** -0.5
    w_out = jax.random.normal(rng_keys[3], (LAYERS, FF, D), jnp.float32) * FF ** -0.5
    return {'tokens': tokens.astype(jnp.bfloat16), 'targets': targets.astype(jnp.bfloat16), 'w_in': w_in.astype(jnp.bfloat16), 'w_out': w_out.astype(jnp.bfloat16)}


def shard_grads(tok_shard, tgt_shard, w_in, w_out):
    inv_total = 1.0 / (SHARDS * TOK)

    def forward_layer(hidden, layer_weights):
        w_first, w_second = layer_weights
        pre_act = jnp.dot(hidden, w_first, preferred_element_type=jnp.float32).astype(jnp.bfloat16)
        post_act = jax.nn.gelu(pre_act.astype(jnp.float32)).astype(jnp.bfloat16)
        branch = jnp.dot(post_act, w_second, preferred_element_type=jnp.float32)
        hidden_next = (hidden.astype(jnp.float32) + branch).astype(jnp.bfloat16)
        return hidden_next, (hidden, pre_act, post_act)

    final, saved = lax.scan(forward_layer, tok_shard, (w_in, w_out))
    grad_top = ((final.astype(jnp.float32) - tgt_shard.astype(jnp.float32)) * inv_total).astype(jnp.bfloat16)

    def backward_layer(grad_hid, layer_data):
        hidden, pre_act, post_act, w_first, w_second = layer_data
        grad_w_out = jnp.dot(post_act.T, grad_hid, preferred_element_type=jnp.float32)
        grad_post = jnp.dot(grad_hid, w_second.T, preferred_element_type=jnp.float32)
        gelu_vjp = jax.vjp(jax.nn.gelu, pre_act.astype(jnp.float32))[1]
        grad_pre = gelu_vjp(grad_post)[0].astype(jnp.bfloat16)
        grad_w_in = jnp.dot(hidden.T, grad_pre, preferred_element_type=jnp.float32)
        through_w = jnp.dot(grad_pre, w_first.T, preferred_element_type=jnp.float32)
        grad_below = (grad_hid.astype(jnp.float32) + through_w).astype(jnp.bfloat16)
        return grad_below, (grad_w_in, grad_w_out)

    hiddens, pre_acts, post_acts = saved
    layer_grads = lax.scan(backward_layer, grad_top, (hiddens, pre_acts, post_acts, w_in, w_out), reverse=True)[1]
    return layer_grads


def reference(tokens, targets, w_in, w_out):
    tok_shards = tokens.reshape(SHARDS, TOK, D)
    tgt_shards = targets.reshape(SHARDS, TOK, D)

    def accumulate(running, shard_pair):
        grad_w_in, grad_w_out = shard_grads(shard_pair[0], shard_pair[1], w_in, w_out)
        return (running[0] + grad_w_in, running[1] + grad_w_out), None

    zero_acc = (jnp.zeros((LAYERS, D, FF), jnp.float32), jnp.zeros((LAYERS, FF, D), jnp.float32))
    totals = lax.scan(accumulate, zero_acc, (tok_shards, tgt_shards))[0]
    return totals[0], totals[1]
```

```python
import jax
import jax.numpy as jnp
from jax import lax
from jax.experimental import pallas as pl
from jax.experimental.pallas import tpu as pltpu
from jax.sharding import PartitionSpec as P

DATA_AXES = ('dy', 'dx')
ROW_CONTRACT = (((0,), (0,)), ((), ()))
COL_CONTRACT = (((1,), (1,)), ((), ()))
F32 = jnp.float32
BF16 = jnp.bfloat16


def send(value, dy_bit, dx_bit):
    pairs = [(d, d ^ (2 * dy_bit + dx_bit)) for d in range(8)]
    return lax.ppermute(value, DATA_AXES, pairs)


def empty(shape, dtype):
    return pl.pallas_call(lambda o: None, out_shape=jax.ShapeDtypeStruct(shape, dtype),
                          out_specs=pl.BlockSpec(memory_space=pl.ANY), name="empty")()


def forward_stack(tokens, w_in, w_out):
    hidden = tokens
    saved = []
    for layer in range(w_in.shape[0]):
        pre_act = jnp.dot(hidden, w_in[layer], preferred_element_type=F32).astype(BF16)
        post_act = jax.nn.gelu(pre_act.astype(F32)).astype(BF16)
        saved.append((hidden, pre_act, post_act))
        branch = jnp.dot(post_act, w_out[layer], preferred_element_type=F32)
        hidden = (hidden.astype(F32) + branch).astype(BF16)
    return hidden, saved


def pre_grad(grad_hid, pre_act, w_second):
    grad_post = lax.dot_general(grad_hid, w_second, COL_CONTRACT, preferred_element_type=F32)
    gelu_vjp = jax.vjp(jax.nn.gelu, pre_act.astype(F32))[1]
    return gelu_vjp(grad_post)[0].astype(BF16)


def input_grad(grad_hid, grad_pre, w_first):
    through_w = lax.dot_general(grad_pre, w_first, COL_CONTRACT, preferred_element_type=F32)
    return (grad_hid.astype(F32) + through_w).astype(BF16)


def piece(left, right, index, rows):
    total = None
    for a, b in zip(left, right):
        part = lax.dot_general(lax.dynamic_slice_in_dim(a, index * rows, rows, 1), b, ROW_CONTRACT,
                               preferred_element_type=F32)
        total = part if total is None else total + part
    return total


def reduce_matrix(left, right, out, layer, x, k):
    rows = left[0].shape[1] // 4
    mine = piece(left, right, 2 * x + k, rows)
    other = piece(left, right, 2 * x + 1 - k, rows)
    chip_sum = mine + send(other, 0, 1)
    final = chip_sum + send(chip_sum, 2, 0)
    across = send(final, 1, 0)
    theirs = send(final, 0, 1)
    theirs_across = send(across, 0, 1)
    for val, idx in ((final, 2 * x + k), (across, 2 * (1 - x) + k), (theirs, 2 * x + 1 - k), (theirs_across, 2 * (1 - x) + 1 - k)):
        out = lax.dynamic_update_slice(out, val[None], (layer, idx * rows, 0))
    return out


def solution(mesh):
    def run(tokens, targets, w_in, w_out):
        inv_total = 1.0 / tokens.shape[0]

        def local_step(tok, tgt, w1, w2):
            n_layers = w1.shape[0]
            x = lax.rem(lax.axis_index('dy'), 2)
            k = lax.axis_index('dx')
            tok_p = send(tok, 1, 0)
            tgt_p = send(tgt, 1, 0)
            sets = []
            for t, y in ((tok, tgt), (tok_p, tgt_p)):
                final, saved = forward_stack(t, w1, w2)
                grad = ((final.astype(F32) - y.astype(F32)) * inv_total).astype(BF16)
                sets.append([grad, saved])
            out_in = empty(w1.shape, F32)
            out_out = empty(w2.shape, F32)
            for layer in reversed(range(n_layers)):
                hid = [s[1][layer][0] for s in sets]
                pre = [s[1][layer][1] for s in sets]
                post = [s[1][layer][2] for s in sets]
                grads = [s[0] for s in sets]
                out_out = reduce_matrix(post, grads, out_out, layer, x, k)
                grad_pre = [pre_grad(g, u, w2[layer]) for g, u in zip(grads, pre)]
                out_in = reduce_matrix(hid, grad_pre, out_in, layer, x, k)
                if layer > 0:
                    for s, g, p in zip(sets, grads, grad_pre):
                        s[0] = input_grad(g, p, w1[layer])
            return out_in, out_out

        data_spec = P(DATA_AXES, None)
        mapped = jax.shard_map(local_step, mesh=mesh, in_specs=(data_spec, data_spec, P(), P()), out_specs=(P(), P()), check_vma=False)
        return mapped(tokens, targets, w_in, w_out)

    return run
```
